32 devices in a mesh: expert: 16 (over z, y, x), half: 2 (over core).
Axes of the slice: x: 2, y: 2, z: 4, core: 2. Of those that a mesh axis runs over, the one named last changes fastest.
Arguments:
- tokens: bfloat16 [1024, 2048], P('expert'), may hold values from -6 to 6
- routes: int32 [1024, 8], P('expert'), may hold values from 0 to 15, all different within a row; in each aligned block of 64 rows (0 to 63, 64 to 127, ...) at most 64 rows name the same one
- gates: float32 [1024, 8], P('expert'), may hold values from 0.05 to 0.5
- cotangent: bfloat16 [1024, 2048], P('expert'), may hold values from -1.5 to 1.5
- w_gate: bfloat16 [16, 2048, 768], P('expert', None, 'half'), may hold values from -0.125 to 0.125
- w_up: bfloat16 [16, 2048, 768], P('expert', None, 'half'), may hold values from -0.125 to 0.125
- w_down: bfloat16 [16, 768, 2048], P('expert', 'half'), may hold values from -0.21875 to 0.21875
Outputs:
- mixed: bfloat16 [1024, 2048], P('expert')
- token_grad: bfloat16 [1024, 2048], P('expert')
- gate_grad: float32 [1024, 8], P('expert')
- grad_gate: bfloat16 [16, 2048, 768], P('expert', None, 'half')
- grad_up: bfloat16 [16, 2048, 768], P('expert', None, 'half')
- grad_down: bfloat16 [16, 768, 2048], P('expert', 'half')
The draws below stay inside these ranges and needn't reach their ends.
Inputs may be any that keep to these rules, and one draw needn't show every extreme that they name: `routes`: each token names 8 different experts. Among the 64 tokens of one index of the expert axis, no expert is named more than 64 times, a bound that some block reaches.
All inputs are finite; a program needn't handle non-finite values.
Results may differ from the reference program's by a relative error of at most 0.0064.
Values may be sent and summed in bfloat16 or wider, within the bound.
No kernel may reach another device: no remote copies, remote signals or barrier semaphores. Data moves between devices by JAX's collectives and lax.ppermute only.
A program may use at most 128 MiB of HBM per device.

```python
import math
import jax
import jax.numpy as jnp
import numpy as np
from jax import lax

D = 2048
HID = 768
TOP = 8
TOK_DEV = 64
EXPERTS = 16
CAP = 64
TOKENS = 1024
N_EXPERT = 16


def level_of(stream_key, shape, shards, low, largest):
    level, own = 1.0, jax.random.fold_in(stream_key, 6)
    for axis_at, shards_of in shards:
        heights = jnp.exp(jax.random.uniform(jax.random.fold_in(own, axis_at), (shards_of,), jnp.float32, low / len(shards), largest / len(shards)))
        level = level * jnp.repeat(heights, shape[axis_at] // shards_of).reshape([-1 if axis == axis_at else 1 for axis in range(len(shape))])
    return level


def shared_out(stream_key, own, number, rows, number_of, top, limit, skew):
    sequence = jax.random.permutation(stream_key, number_of)
    heavy_load, usual = load_shares(number_of, rows * top, limit, skew, True), load_shares(number_of, rows * top, limit, skew, False)
    places = jnp.arange(number_of)

    def named(sizes, rotation):
        used = int((sizes > 0).sum())
        fixed = max(1, used // 4)
        shifted = fixed + (places - fixed + rotation * (used - fixed)) % max(1, number_of - fixed)
        return jnp.zeros((number_of,), jnp.int32).at[sequence[jnp.where(places < fixed, places, shifted)]].set(jnp.asarray(sizes, jnp.int32))

    sizes = jnp.where(number % 4 == 0, named(heavy_load, number // 4), named(usual, number - number // 4 - 1))
    mixed = jax.random.permutation(jax.random.fold_in(own, 3), number_of)
    donor, sink = mixed[0:number_of // 2 * 2:2], mixed[1:number_of // 2 * 2:2]
    room = jnp.minimum(sizes[donor] - 1, limit - sizes[sink]) // 2
    room = jnp.where((donor == sequence[0]) | (sink == sequence[0]) | (sizes[sink] == 0), 0, jnp.maximum(room, 0))
    shifted = jax.random.randint(jax.random.fold_in(own, 4), (number_of // 2,), 0, 1 << 20) % (room + 1)
    sizes = sizes.at[donor].add(-shifted).at[sink].add(shifted)
    items = jnp.searchsorted(jnp.cumsum(sizes), jnp.arange(rows * top), side="right").astype(jnp.int32)
    table = items.reshape(top, rows).T
    table = table[jax.random.permutation(jax.random.fold_in(own, 1), rows)]
    rotation = jax.random.randint(jax.random.fold_in(own, 2), (rows, 1), 0, top)
    return jnp.take_along_axis(table, (jnp.arange(top)[None, :] + rotation) % top, axis=1)


def load_shares(amount, total, bound, slope, full):
    portions = [(1 << 20) // math.isqrt(rank ** slope) + 1 for rank in range(1, amount + 1)]
    largest = bound if full else min(bound, max(-(-total // amount), total * portions[0] // sum(portions)))
    least = 1 if total - largest >= amount - 1 else 0
    given, spare = [largest] + [least] * (amount - 1), total - largest - least * (amount - 1)
    while spare > 0:
        movable = [i for i in range(1, amount) if given[i] < largest] or [i for i in range(1, amount) if given[i] < bound]
        mass, left = sum([portions[i] for i in movable]), spare
        for i in movable:
            extra = min(bound - given[i], max(1, left * portions[i] // mass), spare)
            given[i] = given[i] + extra
            spare = spare - extra
    return np.array(given)


def gaussian(own_key, dims, width, reach, pieces=(), kind=jnp.bfloat16):
    level = level_of(own_key, dims, pieces, -0.22, 0.18) if pieces else 1.0
    array = jax.random.normal(own_key, dims, jnp.float32) * width * level
    return jnp.minimum(jnp.maximum(array, -reach), reach).astype(kind)


def setup_inputs(seed: int = 0) -> dict:
    keys = jax.random.split(jax.random.key(seed), 8)
    tokens = gaussian(keys[0], (TOKENS, D), 1.0, 6.0, ((0, 16),))
    routes_keys = jax.random.split(jax.random.fold_in(keys[1], 1), TOKENS // TOK_DEV)
    routes_turns = jax.random.permutation(jax.random.fold_in(keys[1], 3), TOKENS // TOK_DEV)
    routes = jax.vmap(lambda own, number: shared_out(jax.random.fold_in(keys[1], 2), own, number, TOK_DEV, EXPERTS, TOP, CAP, 2))(routes_keys, routes_turns).reshape((TOKENS, TOP))
    gates = jnp.clip(jnp.exp(math.log(0.5) - 2.3025851 * jax.random.uniform(keys[2], (TOKENS, TOP), jnp.float32) ** level_of(keys[2], (TOKENS, TOP), ((0, 16),), -0.2, 0.2)), 0.05, 0.5)
    cotangent = gaussian(keys[3], (TOKENS, D), 0.25, 1.5, ((0, 16),))
    w_gate = gaussian(keys[4], (EXPERTS, D, HID), D ** -0.5, 0.125, ((0, 16), (2, 2)))
    w_up = gaussian(keys[5], (EXPERTS, D, HID), D ** -0.5, 0.125, ((0, 16), (2, 2)))
    w_down = gaussian(keys[6], (EXPERTS, HID, D), HID ** -0.5, 0.21875, ((0, 16), (1, 2)))
    return dict(tokens=tokens, routes=routes, gates=gates, cotangent=cotangent, w_gate=w_gate, w_up=w_up, w_down=w_down)


def expert_pass(rows, scaled, wgate, wupper, wdown):
    pre_gate = jnp.dot(rows, wgate, preferred_element_type=jnp.float32)
    pre_up = jnp.dot(rows, wupper, preferred_element_type=jnp.float32)
    sigma = jax.nn.sigmoid(pre_gate)
    hidden = (pre_gate * sigma * pre_up).astype(jnp.bfloat16)
    expert_out = jnp.dot(hidden, wdown, preferred_element_type=jnp.float32).astype(jnp.bfloat16)
    back_hidden = jnp.dot(scaled, wdown.T, preferred_element_type=jnp.float32)
    d_up = (back_hidden * pre_gate * sigma).astype(jnp.bfloat16)
    d_gate = (back_hidden * pre_up * sigma * (1.0 + pre_gate * (1.0 - sigma))).astype(jnp.bfloat16)
    slot_grad = jnp.dot(d_gate, wgate.T, preferred_element_type=jnp.float32)
    slot_grad = (slot_grad + jnp.dot(d_up, wupper.T, preferred_element_type=jnp.float32)).astype(jnp.bfloat16)
    grad_gate = jnp.dot(rows.T, d_gate, preferred_element_type=jnp.float32).astype(jnp.bfloat16)
    grad_up = jnp.dot(rows.T, d_up, preferred_element_type=jnp.float32).astype(jnp.bfloat16)
    grad_down = jnp.dot(hidden.T, scaled, preferred_element_type=jnp.float32).astype(jnp.bfloat16)
    return expert_out, slot_grad, grad_gate, grad_up, grad_down


def reference(tokens, routes, gates, cotangent, w_gate, w_up, w_down):
    slot_count = TOK_DEV * TOP
    routed = routes.reshape(N_EXPERT, slot_count).astype(jnp.int32)
    expert_ids = jnp.arange(EXPERTS, dtype=jnp.int32)
    onehot = (routed[:, :, None] == expert_ids[None, None, :]).astype(jnp.int32)
    before = (jnp.cumsum(onehot, axis=1) - onehot).astype(jnp.int32)
    placed = jnp.sum(before * onehot, axis=2).astype(jnp.int32)
    source = jnp.broadcast_to(jnp.arange(N_EXPERT, dtype=jnp.int32)[:, None], routed.shape)
    members = jnp.broadcast_to(jnp.arange(slot_count, dtype=jnp.int32)[None, :], routed.shape)
    slot_table = jnp.full((EXPERTS, N_EXPERT, CAP), slot_count, jnp.int32)
    slot_table = slot_table.at[routed, source, placed].set(members)
    gate_flat = gates.reshape(TOKENS * TOP)
    sources = jnp.arange(N_EXPERT, dtype=jnp.int32)[:, None]

    def one_expert(packed):
        lookup, wgate, wupper, wdown = packed
        present = lookup < slot_count
        clipped = jnp.minimum(lookup, slot_count - 1)
        owners = (sources * TOK_DEV + clipped // TOP).astype(jnp.int32)
        gate_index = (sources * slot_count + clipped).astype(jnp.int32)
        rows = jnp.where(present[:, :, None], tokens[owners], jnp.zeros_like(tokens[owners]))
        weighted = gate_flat[gate_index][:, :, None] * cotangent[owners].astype(jnp.float32)
        scaled = jnp.where(present[:, :, None], weighted, 0.0).astype(jnp.bfloat16)
        return expert_pass(rows.reshape(N_EXPERT * CAP, D), scaled.reshape(N_EXPERT * CAP, D), wgate, wupper, wdown)

    outs_all, grads_all, grad_gate, grad_up, grad_down = lax.map(one_expert, (slot_table, w_gate, w_up, w_down))
    position = (source * CAP + placed).astype(jnp.int32)
    out_slots = outs_all[routed, position].reshape(TOKENS, TOP, D).astype(jnp.float32)
    grad_slots = grads_all[routed, position].reshape(TOKENS, TOP, D).astype(jnp.float32)
    mixed = jnp.sum(gates[:, :, None] * out_slots, axis=1).astype(jnp.bfloat16)
    gate_grad = jnp.sum(cotangent.astype(jnp.float32)[:, None, :] * out_slots, axis=2)
    token_grad = jnp.sum(grad_slots, axis=1).astype(jnp.bfloat16)
    return mixed, token_grad, gate_grad, grad_gate, grad_up, grad_down
```

```python
import jax
import jax.numpy as jnp
from jax import lax
from jax.experimental import pallas as pl
from jax.experimental.pallas import tpu as pltpu
from jax.sharding import PartitionSpec as P


def contract(left, right, left_dim, right_dim):
    return lax.dot_general(
        left, right, (((left_dim,), (right_dim,)), ((), ())), preferred_element_type=jnp.float32
    )


def slot_body(tokens, routes, gates, cotangent, w_gate, w_up, w_down):
    token_count, features = tokens.shape
    top_k = routes.shape[1]
    senders = lax.axis_size("expert")
    halves = lax.axis_size("half")
    experts = w_gate.shape[0] * senders
    slot_count = token_count * top_k
    capacity = 2 * slot_count // experts
    routed = routes.reshape(slot_count)
    onehot = (routed[:, None] == jnp.arange(experts, dtype=jnp.int32)[None, :]).astype(jnp.int32)
    placed = jnp.sum((jnp.cumsum(onehot, axis=0) - onehot) * onehot, axis=1)
    target = routed * capacity + placed
    slot_table = jnp.full((experts * capacity,), slot_count, jnp.int32)
    slot_table = slot_table.at[target].set(jnp.arange(slot_count, dtype=jnp.int32))
    present = slot_table < slot_count
    clipped = jnp.minimum(slot_table, slot_count - 1)
    owners = clipped // top_k
    picked = tokens[owners]
    rows_send = jnp.where(present[:, None], picked, jnp.zeros_like(picked)).reshape(
        experts, capacity, features
    )
    weighted = gates.reshape(slot_count)[clipped][:, None] * cotangent[owners].astype(jnp.float32)
    scaled_send = (
        jnp.where(present[:, None], weighted, 0.0)
        .astype(jnp.bfloat16)
        .reshape(experts, capacity, features)
    )
    half_width = features // halves
    offset = lax.axis_index("half") * half_width
    rows_part = lax.dynamic_slice_in_dim(rows_send, offset, half_width, 2)
    scaled_part = lax.dynamic_slice_in_dim(scaled_send, offset, half_width, 2)
    rows_moved, scaled_moved = (
        lax.all_to_all(rows_part, "expert", split_axis=0, concat_axis=0, tiled=True),
        lax.all_to_all(scaled_part, "expert", split_axis=0, concat_axis=0, tiled=True),
    )
    rows_in, scaled_in = (
        lax.all_gather(rows_moved, "half", axis=2, tiled=True),
        lax.all_gather(scaled_moved, "half", axis=2, tiled=True),
    )
    received = senders * capacity
    rows_in = rows_in.reshape(received, features)
    scaled_in = scaled_in.reshape(received, features)
    wgate = w_gate[0]
    wupper = w_up[0]
    wdown = w_down[0]
    pre_gate = jnp.dot(rows_in, wgate, preferred_element_type=jnp.float32)
    pre_up = jnp.dot(rows_in, wupper, preferred_element_type=jnp.float32)
    sigma = jax.nn.sigmoid(pre_gate)
    hidden = (pre_gate * sigma * pre_up).astype(jnp.bfloat16)
    out_part = jnp.dot(hidden, wdown, preferred_element_type=jnp.float32)
    back_hidden = contract(scaled_in, wdown, 1, 1)
    d_up = (back_hidden * pre_gate * sigma).astype(jnp.bfloat16)
    d_gate = (back_hidden * pre_up * sigma * (1.0 + pre_gate * (1.0 - sigma))).astype(jnp.bfloat16)
    grad_part = contract(d_gate, wgate, 1, 1) + contract(d_up, wupper, 1, 1)
    grad_gate = contract(rows_in, d_gate, 0, 0).astype(jnp.bfloat16)[None]
    grad_up = contract(rows_in, d_up, 0, 0).astype(jnp.bfloat16)[None]
    grad_down = contract(hidden, scaled_in, 0, 0).astype(jnp.bfloat16)[None]
    out_mine, grad_mine = (
        lax.psum_scatter(out_part, "half", scatter_dimension=1, tiled=True),
        lax.psum_scatter(grad_part, "half", scatter_dimension=1, tiled=True),
    )
    out_mine = out_mine.astype(jnp.bfloat16)
    grad_mine = grad_mine.astype(jnp.bfloat16)
    out_block = out_mine.reshape(senders, capacity, features // halves)
    grad_block = grad_mine.reshape(senders, capacity, features // halves)
    out_back, grad_back = (
        lax.all_to_all(out_block, "expert", split_axis=0, concat_axis=0, tiled=True),
        lax.all_to_all(grad_block, "expert", split_axis=0, concat_axis=0, tiled=True),
    )
    out_home, grad_home = (
        lax.all_gather(out_back, "half", axis=2, tiled=True),
        lax.all_gather(grad_back, "half", axis=2, tiled=True),
    )
    out_slots = out_home.reshape(experts * capacity, features)[target].reshape(
        token_count, top_k, features
    )
    grad_slots = grad_home.reshape(experts * capacity, features)[target].reshape(
        token_count, top_k, features
    )
    out_float = out_slots.astype(jnp.float32)
    mixed = jnp.sum(gates[:, :, None] * out_float, axis=1).astype(jnp.bfloat16)
    gate_grad = jnp.sum(cotangent.astype(jnp.float32)[:, None, :] * out_float, axis=2)
    token_grad = jnp.sum(grad_slots.astype(jnp.float32), axis=1).astype(jnp.bfloat16)
    return (mixed, token_grad, gate_grad, grad_gate, grad_up, grad_down)


def rolled(n, step):
    return [((i + 4 * step) % n, i) for i in range(n)]


def flipped(n, bit):
    return [(i, i ^ bit) for i in range(n)]


def swap_half(x):
    return lax.ppermute(x, "half", [(0, 1), (1, 0)])


def near_first(groups):
    return sorted(range(1, groups), key=lambda j: min(j, groups - j))


def stack(*parts):
    return jnp.concatenate(parts, axis=0)


COLOURS = ((1, 2), (2, 1))


def flip(x, n, bit):
    return lax.ppermute(x, "expert", flipped(n, bit))


def after(x, *earlier):
    return lax.optimization_barrier((x, *earlier))[0]


def spread(block, n):
    rows = block.shape[0] // 2
    far_rows = rows * (n // 4 - 1)
    near_rows = rows + far_rows
    shifted = [lax.ppermute(block, "expert", rolled(n, j)) for j in near_first(n // 4)]
    group_one, group_two = [], []
    for colour, (first, second) in enumerate(COLOURS):
        base = colour * 2 * near_rows
        part = slice(colour * rows, (colour + 1) * rows)
        own = block[part]
        far = stack(*[s[part] for s in shifted])
        own_first = flip(own, n, first)
        own_second = flip(stack(own, own_first), n, second)
        far_first = flip(far, n, first)
        far_second = flip(stack(far, far_first), n, second)
        mid = base + near_rows
        group_one += [
            (own, [(base, rows)]),
            (far, [(base + rows, far_rows)]),
            (own_first, [(mid, rows)]),
            (far_first, [(mid + rows, far_rows)]),
        ]
        group_two += [
            (own_second, [(base, rows), (mid, rows)]),
            (far_second, [(base + rows, far_rows), (mid + rows, far_rows)]),
        ]
    return group_one, group_two


def narrow(x):
    return x.astype(jnp.bfloat16)


def wide(x):
    return x.astype(jnp.float32)


def shift_home(block, n, j):
    return lax.ppermute(narrow(block), "expert", [(d, s) for s, d in rolled(n, j)])


def by_colour(x):
    m = x.shape[0] // 2
    return x[:m], x[m:]


def fold(n, kept, sent, which):
    result = []
    for bits, mine, gone in zip(COLOURS, kept, sent):
        moved = flip(narrow(gone), n, bits[which])
        result.append((mine, moved))
    return result


def summed(pairs):
    return [mine + wide(moved) for mine, moved in pairs]


def collect_outputs(one, two, n, held):
    rows = one.shape[0] // n
    near_rows = rows * (n // 4)
    pairs = fold(n, by_colour(one), by_colour(two), 1)
    parts = summed([(mine, after(moved, held)) for mine, moved in pairs])
    runs = [p[at : at + near_rows] for p in parts for at in (0, near_rows)]
    shifted = []
    for at, j in enumerate(near_first(n // 4)):
        block = stack(*[run[(at + 1) * rows : (at + 2) * rows] for run in runs])
        shifted.append(shift_home(block, n, j))
    return stack(*[run[:rows] for run in runs]), shifted


def finish_outputs(kept, shifted, n, held):
    total = kept
    for moved in shifted:
        total = total + wide(after(moved, held))
    halves = [by_colour(part) for part in by_colour(total)]
    return narrow(stack(*summed(fold(n, *zip(*halves), 0))))


def collect_gradients(one, two, n):
    rows = one.shape[0] // n
    near_rows = rows * (n // 4)

    def far(x):
        return stack(x[rows:near_rows], x[near_rows + rows :])

    def own(x):
        return stack(x[:rows], x[near_rows : near_rows + rows])

    ones, twos = by_colour(one), by_colour(two)
    far_pairs = fold(n, [far(x) for x in ones], [far(x) for x in twos], 1)
    own_pairs = fold(n, [own(x) for x in ones], [own(x) for x in twos], 1)
    far_pairs = fold(n, *zip(*[by_colour(x) for x in summed(far_pairs)]), 0)
    fars = summed(far_pairs)
    own_pairs = fold(n, *zip(*[by_colour(x) for x in summed(own_pairs)]), 0)
    mark = own_pairs[1][1]
    total = stack(*summed(own_pairs))
    shifted = []
    for at, j in enumerate(near_first(n // 4)):
        block = stack(*[part[at * rows : (at + 1) * rows] for part in fars])
        shifted.append(shift_home(block, n, j))
    return total, shifted, mark


VMEM = pl.BlockSpec(memory_space=pltpu.VMEM)
SMEM = pl.BlockSpec(memory_space=pltpu.SMEM)


def size_of(x):
    return x.size * x.dtype.itemsize


def whole(kernel, out_shapes, args, scalars=0, flops=0):
    moved = sum(size_of(x) for x in jax.tree.leaves((args, out_shapes)))
    return pl.pallas_call(
        kernel,
        out_shape=out_shapes,
        in_specs=[SMEM] * scalars + [VMEM] * (len(args) - scalars),
        out_specs=jax.tree.map(lambda _: VMEM, out_shapes),
        cost_estimate=pl.CostEstimate(flops=flops, bytes_accessed=moved, transcendentals=0),
        compiler_params=pltpu.CompilerParams(vmem_limit_bytes=moved + 4 * 2**20),
    )(*args)


def assemble(placed):
    parts, places = zip(*placed)

    def kernel(*refs):
        out = refs[-1]
        for ref, runs in zip(refs[:-1], places):
            at = 0
            for start, count in runs:
                out[start : start + count] = ref[at : at + count]
                at += count

    total = sum(p.shape[0] for p in parts)
    shape = jax.ShapeDtypeStruct((total, parts[0].shape[1]), parts[0].dtype)
    return whole(kernel, shape, parts, 0, 1000 * total)


def product_over_rows(left, right, tall=None):
    groups = len(left)
    tile = 256
    rows, width = right[0].shape

    def kernel(*refs):
        def joined(k):
            return jnp.concatenate([ref[...] for ref in refs[k * groups : (k + 1) * groups]], 0)

        both = narrow(contract(joined(0), joined(1), 0, 0))
        outs = refs[2 * groups :]
        for at, out in enumerate(outs):
            m = both.shape[1] // len(outs)
            out[0] = both[:, at * m : (at + 1) * m]

    def fixed(cols):
        return [pl.BlockSpec((rows, cols), lambda i: (0, 0))] * groups

    def moving():
        return [pl.BlockSpec((rows, tile), lambda i: (0, i))] * groups

    if tall is None:
        unit, features = left[0].shape[1], width
        in_specs = fixed(unit) + moving()
        out_shape = [jax.ShapeDtypeStruct((1, unit, features), jnp.bfloat16)]
        out_specs = [pl.BlockSpec((1, unit, tile), lambda i: (0, 0, i))]
        flops = 2 * groups * rows * unit * features
    else:
        unit = width // 2
        features = tall
        in_specs = moving() + fixed(width)
        out_shape = [jax.ShapeDtypeStruct((1, features, unit), jnp.bfloat16)] * 2
        out_specs = [pl.BlockSpec((1, tile, unit), lambda i: (0, i, 0))] * 2
        flops = 2 * groups * rows * width * features
    return pl.pallas_call(
        kernel,
        grid=(features // tile,),
        out_shape=out_shape,
        in_specs=in_specs,
        out_specs=out_specs,
        cost_estimate=pl.CostEstimate(flops=flops, bytes_accessed=0, transcendentals=0),
        compiler_params=pltpu.CompilerParams(vmem_limit_bytes=14 * 2**20),
    )(*left, *right)


def blocks_of(rows, step, work):
    def one(i, carry):
        work(pl.ds(pl.multiple_of(i * step, step), step))
        return carry

    lax.fori_loop(0, rows // step, one, 0)


def gate_of(side, experts, me):
    lanes = lax.broadcasted_iota(jnp.int32, side.shape, 1)
    named = (lax.rem(lanes, experts) == me) & (lanes < 3 * experts)
    return jnp.sum(jnp.where(named, side.astype(jnp.float32), 0.0), axis=1, keepdims=True)


def forward(rows_in, w_in, w_down, where, experts, out_dtype):
    rows = rows_in.shape[0]
    features, width = w_in.shape
    unit = width // 2

    def kernel(where_ref, x_ref, win_ref, down_ref, pre_ref, weighted_ref, out_ref):
        me = where_ref[0]

        def work(at):
            pre = jnp.dot(
                x_ref[at, :features], win_ref[...], preferred_element_type=jnp.float32
            )
            pre_ref[at, :] = pre
            gate = gate_of(x_ref[at, features:], experts, me)
            pre_gate = pre[:, :unit]
            hidden = pre_gate * jax.nn.sigmoid(pre_gate) * pre[:, unit:]
            weighted = (gate * hidden).astype(jnp.bfloat16)
            weighted_ref[at, :] = weighted
            out_ref[at, :] = jnp.dot(
                weighted, down_ref[...], preferred_element_type=jnp.float32
            ).astype(out_dtype)

        blocks_of(rows, min(rows, 256), work)

    shapes = (
        jax.ShapeDtypeStruct((rows, width), jnp.float32),
        jax.ShapeDtypeStruct((rows, unit), jnp.bfloat16),
        jax.ShapeDtypeStruct((rows, features), out_dtype),
    )
    return whole(kernel, shapes, (where, rows_in, w_in, w_down), 1, 3 * rows * features * width)


def backward(cot, rows_in, pre, w_in, w_down, where, experts, halves, out_dtype):
    rows, features = cot.shape
    width = w_in.shape[1]
    unit = width // 2
    back_width = -(-3 * halves * experts // 128) * 128

    def kernel(where_ref, cot_ref, side_ref, pre_ref, win_ref, down_ref, d_ref, out_ref):
        me, half = where_ref[0], where_ref[1]

        def work(at):
            back = lax.dot_general(
                cot_ref[at, :],
                down_ref[...],
                (((1,), (1,)), ((), ())),
                preferred_element_type=jnp.float32,
            )
            gate = gate_of(side_ref[at, features:], experts, me)
            pre_gate, pre_up = pre_ref[at, :unit], pre_ref[at, unit:]
            sigma = jax.nn.sigmoid(pre_gate)
            act = pre_gate * sigma
            product = jnp.where(gate > 0.0, act * pre_up * back, 0.0)
            gate_part = jnp.sum(product, axis=1, keepdims=True)
            back = gate * back
            d_ref[at, unit:] = (back * act).astype(jnp.bfloat16)
            d_ref[at, :unit] = (back * pre_up * sigma * (1.0 + pre_gate * (1.0 - sigma))).astype(
                jnp.bfloat16
            )
            out_ref[at, :features] = lax.dot_general(
                d_ref[at, :],
                win_ref[...],
                (((1,), (1,)), ((), ())),
                preferred_element_type=jnp.float32,
            ).astype(out_dtype)
            high = gate_part.astype(jnp.bfloat16).astype(jnp.float32)
            rest = gate_part - high
            middle = rest.astype(jnp.bfloat16).astype(jnp.float32)
            lanes = lax.broadcasted_iota(jnp.int32, (gate_part.shape[0], back_width), 1)
            side = jnp.zeros(lanes.shape, jnp.float32)
            for i, piece in enumerate((high, middle, rest - middle)):
                side = jnp.where(lanes == (i * halves + half) * experts + me, piece, side)
            out_ref[at, features:] = side.astype(out_dtype)

        blocks_of(rows, min(rows, 256), work)

    shapes = (
        jax.ShapeDtypeStruct((rows, width), jnp.bfloat16),
        jax.ShapeDtypeStruct((rows, features + back_width), out_dtype),
    )
    operands = (where, cot, rows_in, pre, w_in, w_down)
    return whole(kernel, shapes, operands, 1, 3 * rows * features * width)


def pieces(x):
    high = lax.reduce_precision(x, 8, 7)
    rest = x - high
    middle = lax.reduce_precision(rest, 8, 7)
    return [high, middle, rest - middle]


def dense_body(tokens, routes, gates, cotangent, w_gate, w_up, w_down):
    token_count, features = tokens.shape
    senders = lax.axis_size("expert")
    halves = lax.axis_size("half")
    experts = w_gate.shape[0] * senders
    me = lax.axis_index("expert")
    half = lax.axis_index("half")
    rows = token_count // halves
    bf16, f32 = jnp.bfloat16, jnp.float32

    def padded(x):
        return jnp.pad(x, ((0, 0), (0, -x.shape[1] % 128)))

    def mine(x):
        return lax.dynamic_slice_in_dim(x, half * rows, rows, 0)

    onehot = routes[:, :, None] == jnp.arange(experts, dtype=jnp.int32)[None, None, :]
    by_expert = jnp.sum(jnp.where(onehot, gates[:, :, None], 0.0), axis=1)
    side = padded(jnp.concatenate(pieces(by_expert), axis=1)).astype(bf16)
    where = jnp.stack([me, half]).astype(jnp.int32)
    w_in = jnp.concatenate([w_gate[0], w_up[0]], axis=1)
    w_out = w_down[0]

    lower = half == 0
    block = mine(jnp.concatenate([tokens, side], axis=1))
    block, lower, where = lax.optimization_barrier((block, lower, where))
    tok_one, tok_two = spread(block, senders)
    cot_one, cot_two = spread(mine(cotangent), senders)
    sums, saved = {}, {}
    for tag, placed in (("f", tok_one), ("s", tok_two)):
        rows_mine = assemble(placed)
        rows_other = swap_half(rows_mine)
        pre, weighted, out_mine = forward(rows_mine, w_in, w_out, where, experts, f32)
        pre_o, weighted_o, out_other = forward(rows_other, w_in, w_out, where, experts, bf16)
        sums[tag] = out_mine + wide(swap_half(out_other))
        saved[tag] = [(rows_mine, pre, weighted), (rows_other, pre_o, weighted_o)]

    all_rows, all_d, all_weighted, all_cots = [], [], [], []
    slot_sums = {}
    for tag, placed in (("f", cot_one), ("s", cot_two)):
        cot_mine = assemble(placed)
        cot_other = swap_half(cot_mine)
        slots = []
        for cot, kept, dtype in ((cot_mine, saved[tag][0], f32), (cot_other, saved[tag][1], bf16)):
            rows_in, pre, weighted = kept
            d, slot = backward(
                cot, rows_in, pre, w_in, w_out, where, experts, halves, dtype
            )
            slots.append(slot)
            all_rows.append(rows_in)
            all_d.append(d)
            all_weighted.append(weighted)
            all_cots.append(cot)
        slot_other = swap_half(slots[1])
        slot_sums[tag] = slots[0] + wide(slot_other)

    mix_kept, mix_shifted = collect_outputs(sums["f"], sums["s"], senders, slot_other)
    grad_home, grad_shifted, mark = collect_gradients(slot_sums["f"], slot_sums["s"], senders)
    mixed = finish_outputs(mix_kept, mix_shifted, senders, mark)
    (grad_down,) = product_over_rows(all_weighted, all_cots)
    grad_gate, grad_up = product_over_rows(all_rows, all_d, features)

    def both(x, other):
        return jnp.where(lower, stack(x, other), stack(other, x))

    mixed = both(mixed, swap_half(mixed))
    for moved in grad_shifted:
        grad_home = grad_home + wide(after(moved, mixed))
    grad_home = narrow(grad_home)
    grad_other = swap_half(grad_home)
    token_grad = both(grad_home[:, :features], grad_other[:, :features])
    by_expert = both(grad_home[:, features:], grad_other[:, features:]).astype(f32)
    by_expert = by_expert[:, : 3 * halves * experts].reshape(token_count, 3 * halves, experts)
    by_expert = jnp.sum(by_expert, axis=1)
    gate_grad = jnp.sum(jnp.where(onehot, by_expert[:, None, :], 0.0), axis=2)
    return (mixed, token_grad, gate_grad, grad_gate, grad_up, grad_down)


def body(tokens, routes, gates, cotangent, w_gate, w_up, w_down):
    token_count, top_k = routes.shape
    senders = lax.axis_size("expert")
    halves = lax.axis_size("half")
    capacity = 2 * token_count * top_k // (w_gate.shape[0] * senders)
    dense = capacity >= token_count and w_gate.shape[0] == 1
    if dense and halves == 2 and senders % 4 == 0 and token_count % 32 == 0:
        return dense_body(tokens, routes, gates, cotangent, w_gate, w_up, w_down)
    return slot_body(tokens, routes, gates, cotangent, w_gate, w_up, w_down)


def solution(mesh):
    placed = (
        P("expert", None),
        P("expert", None),
        P("expert", None),
        P("expert", None),
        P("expert", None, "half"),
        P("expert", None, "half"),
        P("expert", "half", None),
    )
    return jax.shard_map(
        body,
        mesh=mesh,
        in_specs=placed,
        out_specs=(
            P("expert", None),
            P("expert", None),
            P("expert", None),
            P("expert", None, "half"),
            P("expert", None, "half"),
            P("expert", "half", None),
        ),
        check_vma=False,
    )
```

```python
import jax
import jax.numpy as jnp
from jax import lax
from jax.experimental import pallas as pl
from jax.experimental.pallas import tpu as pltpu
from jax.sharding import PartitionSpec as P


def contract(left, right, left_dim, right_dim):
    return lax.dot_general(
        left, right, (((left_dim,), (right_dim,)), ((), ())), preferred_element_type=jnp.float32
    )


def slot_body(tokens, routes, gates, cotangent, w_gate, w_up, w_down):
    token_count, features = tokens.shape
    top_k = routes.shape[1]
    senders = lax.axis_size("expert")
    halves = lax.axis_size("half")
    experts = w_gate.shape[0] * senders
    slot_count = token_count * top_k
    capacity = 2 * slot_count // experts
    routed = routes.reshape(slot_count)
    onehot = (routed[:, None] == jnp.arange(experts, dtype=jnp.int32)[None, :]).astype(jnp.int32)
    placed = jnp.sum((jnp.cumsum(onehot, axis=0) - onehot) * onehot, axis=1)
    target = routed * capacity + placed
    slot_table = jnp.full((experts * capacity,), slot_count, jnp.int32)
    slot_table = slot_table.at[target].set(jnp.arange(slot_count, dtype=jnp.int32))
    present = slot_table < slot_count
    clipped = jnp.minimum(slot_table, slot_count - 1)
    owners = clipped // top_k
    picked = tokens[owners]
    rows_send = jnp.where(present[:, None], picked, jnp.zeros_like(picked)).reshape(
        experts, capacity, features
    )
    weighted = gates.reshape(slot_count)[clipped][:, None] * cotangent[owners].astype(jnp.float32)
    scaled_send = (
        jnp.where(present[:, None], weighted, 0.0)
        .astype(jnp.bfloat16)
        .reshape(experts, capacity, features)
    )
    half_width = features // halves
    offset = lax.axis_index("half") * half_width
    rows_part = lax.dynamic_slice_in_dim(rows_send, offset, half_width, 2)
    scaled_part = lax.dynamic_slice_in_dim(scaled_send, offset, half_width, 2)
    rows_moved, scaled_moved = (
        lax.all_to_all(rows_part, "expert", split_axis=0, concat_axis=0, tiled=True),
        lax.all_to_all(scaled_part, "expert", split_axis=0, concat_axis=0, tiled=True),
    )
    rows_in, scaled_in = (
        lax.all_gather(rows_moved, "half", axis=2, tiled=True),
        lax.all_gather(scaled_moved, "half", axis=2, tiled=True),
    )
    received = senders * capacity
    rows_in = rows_in.reshape(received, features)
    scaled_in = scaled_in.reshape(received, features)
    wgate = w_gate[0]
    wupper = w_up[0]
    wdown = w_down[0]
    pre_gate = jnp.dot(rows_in, wgate, preferred_element_type=jnp.float32)
    pre_up = jnp.dot(rows_in, wupper, preferred_element_type=jnp.float32)
    sigma = jax.nn.sigmoid(pre_gate)
    hidden = (pre_gate * sigma * pre_up).astype(jnp.bfloat16)
    out_part = jnp.dot(hidden, wdown, preferred_element_type=jnp.float32)
    back_hidden = contract(scaled_in, wdown, 1, 1)
    d_up = (back_hidden * pre_gate * sigma).astype(jnp.bfloat16)
    d_gate = (back_hidden * pre_up * sigma * (1.0 + pre_gate * (1.0 - sigma))).astype(jnp.bfloat16)
    grad_part = contract(d_gate, wgate, 1, 1) + contract(d_up, wupper, 1, 1)
    grad_gate = contract(rows_in, d_gate, 0, 0).astype(jnp.bfloat16)[None]
    grad_up = contract(rows_in, d_up, 0, 0).astype(jnp.bfloat16)[None]
    grad_down = contract(hidden, scaled_in, 0, 0).astype(jnp.bfloat16)[None]
    out_mine, grad_mine = (
        lax.psum_scatter(out_part, "half", scatter_dimension=1, tiled=True),
        lax.psum_scatter(grad_part, "half", scatter_dimension=1, tiled=True),
    )
    out_mine = out_mine.astype(jnp.bfloat16)
    grad_mine = grad_mine.astype(jnp.bfloat16)
    out_block = out_mine.reshape(senders, capacity, features // halves)
    grad_block = grad_mine.reshape(senders, capacity, features // halves)
    out_back, grad_back = (
        lax.all_to_all(out_block, "expert", split_axis=0, concat_axis=0, tiled=True),
        lax.all_to_all(grad_block, "expert", split_axis=0, concat_axis=0, tiled=True),
    )
    out_home, grad_home = (
        lax.all_gather(out_back, "half", axis=2, tiled=True),
        lax.all_gather(grad_back, "half", axis=2, tiled=True),
    )
    out_slots = out_home.reshape(experts * capacity, features)[target].reshape(
        token_count, top_k, features
    )
    grad_slots = grad_home.reshape(experts * capacity, features)[target].reshape(
        token_count, top_k, features
    )
    out_float = out_slots.astype(jnp.float32)
    mixed = jnp.sum(gates[:, :, None] * out_float, axis=1).astype(jnp.bfloat16)
    gate_grad = jnp.sum(cotangent.astype(jnp.float32)[:, None, :] * out_float, axis=2)
    token_grad = jnp.sum(grad_slots.astype(jnp.float32), axis=1).astype(jnp.bfloat16)
    return (mixed, token_grad, gate_grad, grad_gate, grad_up, grad_down)


def rolled(n, step):
    return [((i + 4 * step) % n, i) for i in range(n)]


def flipped(n, bit):
    return [(i, i ^ bit) for i in range(n)]


def swap_half(x):
    return lax.ppermute(x, "half", [(0, 1), (1, 0)])


def near_first(groups):
    return sorted(range(1, groups), key=lambda j: min(j, groups - j))


def stack(*parts):
    return jnp.concatenate(parts, axis=0)


COLOURS = ((1, 2), (2, 1))


def flip(x, n, bit):
    return lax.ppermute(x, "expert", flipped(n, bit))


def after(x, *earlier):
    return lax.optimization_barrier((x, *earlier))[0]


def spread(block, n):
    rows = block.shape[0] // 2
    far_rows = rows * (n // 4 - 1)
    near_rows = rows + far_rows
    shifted = [lax.ppermute(block, "expert", rolled(n, j)) for j in near_first(n // 4)]
    group_one, group_two = [], []
    for colour, (first, second) in enumerate(COLOURS):
        base = colour * 2 * near_rows
        part = slice(colour * rows, (colour + 1) * rows)
        own = block[part]
        far = stack(*[s[part] for s in shifted])
        own_first = flip(own, n, first)
        own_second = flip(stack(own, own_first), n, second)
        far_first = flip(far, n, first)
        far_second = flip(stack(far, far_first), n, second)
        mid = base + near_rows
        group_one += [
            (own, [(base, rows)]),
            (far, [(base + rows, far_rows)]),
            (own_first, [(mid, rows)]),
            (far_first, [(mid + rows, far_rows)]),
        ]
        group_two += [
            (own_second, [(base, rows), (mid, rows)]),
            (far_second, [(base + rows, far_rows), (mid + rows, far_rows)]),
        ]
    return group_one, group_two


def narrow(x):
    return x.astype(jnp.bfloat16)


def wide(x):
    return x.astype(jnp.float32)


def shift_home(block, n, j):
    return lax.ppermute(narrow(block), "expert", [(d, s) for s, d in rolled(n, j)])


def by_colour(x):
    m = x.shape[0] // 2
    return x[:m], x[m:]


def fold(n, kept, sent, which):
    result = []
    for bits, mine, gone in zip(COLOURS, kept, sent):
        moved = flip(narrow(gone), n, bits[which])
        result.append((mine, moved))
    return result


def summed(pairs):
    return [mine + wide(moved) for mine, moved in pairs]


def collect_outputs(one, two, n, held):
    rows = one.shape[0] // n
    near_rows = rows * (n // 4)
    pairs = fold(n, by_colour(one), by_colour(two), 1)
    parts = summed([(mine, after(moved, held)) for mine, moved in pairs])
    runs = [p[at : at + near_rows] for p in parts for at in (0, near_rows)]
    *others, farthest = enumerate(near_first(n // 4))
    shifted = []
    for at, j in others:
        block = stack(*[run[(at + 1) * rows : (at + 2) * rows] for run in runs])
        shifted.append(shift_home(block, n, j))
    at, j = farthest
    ends = [run[(at + 1) * rows : (at + 2) * rows] for run in runs]
    ends = stack(*summed(fold(n, ends[0::2], ends[1::2], 0)))
    last = shift_home(ends, n, j)
    return stack(*[run[:rows] for run in runs]), shifted, last


def finish_outputs(kept, shifted, last, n, held):
    total = kept
    for moved in shifted:
        total = total + wide(after(moved, held))
    halves = [by_colour(part) for part in by_colour(total)]
    total = stack(*summed(fold(n, *zip(*halves), 0)))
    return narrow(total + wide(after(last, held)))


def collect_gradients(one, two, n):
    rows = one.shape[0] // n
    near_rows = rows * (n // 4)

    def far(x):
        return stack(x[rows:near_rows], x[near_rows + rows :])

    def own(x):
        return stack(x[:rows], x[near_rows : near_rows + rows])

    ones, twos = by_colour(one), by_colour(two)
    far_pairs = fold(n, [far(x) for x in ones], [far(x) for x in twos], 1)
    own_pairs = fold(n, [own(x) for x in ones], [own(x) for x in twos], 1)
    far_pairs = fold(n, *zip(*[by_colour(x) for x in summed(far_pairs)]), 0)
    mark = far_pairs[1][1]
    fars = summed(far_pairs)
    own_pairs = fold(n, *zip(*[by_colour(x) for x in summed(own_pairs)]), 0)
    total = stack(*summed(own_pairs))
    shifted = []
    for at, j in enumerate(near_first(n // 4)):
        block = stack(*[part[at * rows : (at + 1) * rows] for part in fars])
        shifted.append(shift_home(block, n, j))
    return total, shifted, mark


VMEM = pl.BlockSpec(memory_space=pltpu.VMEM)
SMEM = pl.BlockSpec(memory_space=pltpu.SMEM)


def size_of(x):
    return x.size * x.dtype.itemsize


def whole(kernel, out_shapes, args, scalars=0):
    moved = sum(size_of(x) for x in jax.tree.leaves((args, out_shapes)))
    return pl.pallas_call(
        kernel,
        out_shape=out_shapes,
        in_specs=[SMEM] * scalars + [VMEM] * (len(args) - scalars),
        out_specs=jax.tree.map(lambda _: VMEM, out_shapes),
        cost_estimate=pl.CostEstimate(flops=1000, bytes_accessed=moved, transcendentals=0),
        compiler_params=pltpu.CompilerParams(vmem_limit_bytes=moved + 4 * 2**20),
    )(*args)


def assemble(placed):
    parts, places = zip(*placed)

    def kernel(*refs):
        out = refs[-1]
        for ref, runs in zip(refs[:-1], places):
            at = 0
            for start, count in runs:
                out[start : start + count] = ref[at : at + count]
                at += count

    total = sum(p.shape[0] for p in parts)
    shape = jax.ShapeDtypeStruct((total, parts[0].shape[1]), parts[0].dtype)
    return whole(kernel, shape, parts, 0)


def add_rows(x, y):
    def kernel(x_ref, y_ref, out_ref):
        out_ref[...] = x_ref[...] + wide(y_ref[...])

    return whole(kernel, jax.ShapeDtypeStruct(x.shape, x.dtype), (x, y))


def product_over_rows(left, right, tall=None):
    groups = len(left)
    rows, width = right[0].shape
    tile = 256 if tall else max(t for t in (128, 256, 512, 1024) if width % t == 0)

    def kernel(*refs):
        def joined(k):
            return jnp.concatenate([ref[...] for ref in refs[k * groups : (k + 1) * groups]], 0)

        both = narrow(contract(joined(0), joined(1), 0, 0))
        outs = refs[2 * groups :]
        for at, out in enumerate(outs):
            m = both.shape[1] // len(outs)
            out[0] = both[:, at * m : (at + 1) * m]

    def fixed(cols):
        return [pl.BlockSpec((rows, cols), lambda i: (0, 0))] * groups

    def moving():
        return [pl.BlockSpec((rows, tile), lambda i: (0, i))] * groups

    if tall is None:
        unit, features = left[0].shape[1], width
        in_specs = fixed(unit) + moving()
        out_shape = [jax.ShapeDtypeStruct((1, unit, features), jnp.bfloat16)]
        out_specs = [pl.BlockSpec((1, unit, tile), lambda i: (0, 0, i))]
    else:
        unit = width // 2
        features = tall
        in_specs = moving() + fixed(width)
        out_shape = [jax.ShapeDtypeStruct((1, features, unit), jnp.bfloat16)] * 2
        out_specs = [pl.BlockSpec((1, tile, unit), lambda i: (0, i, 0))] * 2
    return pl.pallas_call(
        kernel,
        grid=(features // tile,),
        out_shape=out_shape,
        in_specs=in_specs,
        out_specs=out_specs,
        cost_estimate=pl.CostEstimate(flops=1000, bytes_accessed=0, transcendentals=0),
        compiler_params=pltpu.CompilerParams(vmem_limit_bytes=14 * 2**20),
    )(*left, *right)


def blocks_of(rows, step, work):
    def one(i, carry):
        work(pl.ds(pl.multiple_of(i * step, step), step))
        return carry

    lax.fori_loop(0, rows // step, one, 0)


def gate_of(side, experts, me):
    lanes = lax.broadcasted_iota(jnp.int32, side.shape, 1)
    named = (lax.rem(lanes, experts) == me) & (lanes < 3 * experts)
    return jnp.sum(jnp.where(named, side.astype(jnp.float32), 0.0), axis=1, keepdims=True)


def forward(rows_in, w_in, w_down, where, experts, out_dtype):
    rows = rows_in.shape[0]
    features, width = w_in.shape
    unit = width // 2

    def kernel(where_ref, x_ref, win_ref, down_ref, pre_ref, weighted_ref, out_ref):
        me = where_ref[0]

        def work(at):
            pre = jnp.dot(
                x_ref[at, :features], win_ref[...], preferred_element_type=jnp.float32
            )
            pre_ref[at, :] = pre
            gate = gate_of(x_ref[at, features:], experts, me)
            pre_gate = pre[:, :unit]
            hidden = pre_gate * jax.nn.sigmoid(pre_gate) * pre[:, unit:]
            weighted = (gate * hidden).astype(jnp.bfloat16)
            weighted_ref[at, :] = weighted
            out_ref[at, :] = jnp.dot(
                weighted, down_ref[...], preferred_element_type=jnp.float32
            ).astype(out_dtype)

        blocks_of(rows, min(rows, 256), work)

    shapes = (
        jax.ShapeDtypeStruct((rows, width), jnp.float32),
        jax.ShapeDtypeStruct((rows, unit), jnp.bfloat16),
        jax.ShapeDtypeStruct((rows, features), out_dtype),
    )
    return whole(kernel, shapes, (where, rows_in, w_in, w_down), 1)


def backward(cot, rows_in, pre, w_in, w_down, where, experts, halves, out_dtype):
    rows, features = cot.shape
    width = w_in.shape[1]
    unit = width // 2
    back_width = -(-3 * halves * experts // 128) * 128

    def kernel(where_ref, cot_ref, side_ref, pre_ref, win_ref, down_ref, d_ref, out_ref):
        me, half = where_ref[0], where_ref[1]

        def work(at):
            back = lax.dot_general(
                cot_ref[at, :],
                down_ref[...],
                (((1,), (1,)), ((), ())),
                preferred_element_type=jnp.float32,
            )
            gate = gate_of(side_ref[at, features:], experts, me)
            pre_gate, pre_up = pre_ref[at, :unit], pre_ref[at, unit:]
            sigma = jax.nn.sigmoid(pre_gate)
            act = pre_gate * sigma
            product = jnp.where(gate > 0.0, act * pre_up * back, 0.0)
            gate_part = jnp.sum(product, axis=1, keepdims=True)
            back = gate * back
            d_ref[at, unit:] = (back * act).astype(jnp.bfloat16)
            d_ref[at, :unit] = (back * pre_up * sigma * (1.0 + pre_gate * (1.0 - sigma))).astype(
                jnp.bfloat16
            )
            out_ref[at, :features] = lax.dot_general(
                d_ref[at, :],
                win_ref[...],
                (((1,), (1,)), ((), ())),
                preferred_element_type=jnp.float32,
            ).astype(out_dtype)
            high = gate_part.astype(jnp.bfloat16).astype(jnp.float32)
            rest = gate_part - high
            middle = rest.astype(jnp.bfloat16).astype(jnp.float32)
            lanes = lax.broadcasted_iota(jnp.int32, (gate_part.shape[0], back_width), 1)
            side = jnp.zeros(lanes.shape, jnp.float32)
            for i, piece in enumerate((high, middle, rest - middle)):
                side = jnp.where(lanes == (i * halves + half) * experts + me, piece, side)
            out_ref[at, features:] = side.astype(out_dtype)

        blocks_of(rows, min(rows, 256), work)

    shapes = (
        jax.ShapeDtypeStruct((rows, width), jnp.bfloat16),
        jax.ShapeDtypeStruct((rows, features + back_width), out_dtype),
    )
    operands = (where, cot, rows_in, pre, w_in, w_down)
    return whole(kernel, shapes, operands, 1)


def pieces(x):
    high = lax.reduce_precision(x, 8, 7)
    rest = x - high
    middle = lax.reduce_precision(rest, 8, 7)
    return [high, middle, rest - middle]


def dense_body(tokens, routes, gates, cotangent, w_gate, w_up, w_down):
    token_count, features = tokens.shape
    senders = lax.axis_size("expert")
    halves = lax.axis_size("half")
    experts = w_gate.shape[0] * senders
    me = lax.axis_index("expert")
    half = lax.axis_index("half")
    rows = token_count // halves
    bf16, f32 = jnp.bfloat16, jnp.float32

    def padded(x):
        return jnp.pad(x, ((0, 0), (0, -x.shape[1] % 128)))

    def mine(x):
        return lax.dynamic_slice_in_dim(x, half * rows, rows, 0)

    onehot = routes[:, :, None] == jnp.arange(experts, dtype=jnp.int32)[None, None, :]
    by_expert = jnp.sum(jnp.where(onehot, gates[:, :, None], 0.0), axis=1)
    side = padded(jnp.concatenate(pieces(by_expert), axis=1)).astype(bf16)
    where = jnp.stack([me, half]).astype(jnp.int32)
    w_in = jnp.concatenate([w_gate[0], w_up[0]], axis=1)
    w_out = w_down[0]

    lower = half == 0
    block = mine(jnp.concatenate([tokens, side], axis=1))
    block, lower, where = lax.optimization_barrier((block, lower, where))
    tok_one, tok_two = spread(block, senders)
    cot_one, cot_two = spread(mine(cotangent), senders)
    sums, saved = {}, {}
    for tag, placed in (("f", tok_one), ("s", tok_two)):
        rows_mine = assemble(placed)
        rows_other = swap_half(rows_mine)
        pre, weighted, out_mine = forward(rows_mine, w_in, w_out, where, experts, f32)
        pre_o, weighted_o, out_other = forward(rows_other, w_in, w_out, where, experts, bf16)
        sums[tag] = out_mine + wide(swap_half(out_other))
        saved[tag] = [(rows_mine, pre, weighted), (rows_other, pre_o, weighted_o)]

    all_rows, all_d, all_weighted, all_cots = [], [], [], []
    slot_sums = {}
    for tag, placed in (("f", cot_one), ("s", cot_two)):
        cot_mine = assemble(placed)
        cot_other = swap_half(cot_mine)
        slots = []
        for cot, kept, dtype in ((cot_mine, saved[tag][0], f32), (cot_other, saved[tag][1], bf16)):
            rows_in, pre, weighted = kept
            d, slot = backward(
                cot, rows_in, pre, w_in, w_out, where, experts, halves, dtype
            )
            slots.append(slot)
            all_rows.append(rows_in)
            all_d.append(d)
            all_weighted.append(weighted)
            all_cots.append(cot)
        slot_other = swap_half(slots[1])
        if tag == "f":
            slot_sums[tag] = add_rows(slots[0], slot_other)
        else:
            slot_sums[tag] = slots[0] + wide(slot_other)

    mix_parts = collect_outputs(sums["f"], sums["s"], senders, slot_other)
    grad_home, grad_shifted, mark = collect_gradients(slot_sums["f"], slot_sums["s"], senders)
    mixed = finish_outputs(*mix_parts, senders, mark)
    (grad_down,) = product_over_rows(all_weighted, all_cots)
    grad_gate, grad_up = product_over_rows(all_rows, all_d, features)

    def both(x, other):
        return jnp.where(lower, stack(x, other), stack(other, x))

    mixed = both(mixed, swap_half(mixed))
    for moved in grad_shifted:
        grad_home = grad_home + wide(moved)
    grad_home = narrow(grad_home)
    grad_other = swap_half(grad_home)
    token_grad = both(grad_home[:, :features], grad_other[:, :features])
    by_expert = both(grad_home[:, features:], grad_other[:, features:]).astype(f32)
    by_expert = by_expert[:, : 3 * halves * experts].reshape(token_count, 3 * halves, experts)
    by_expert = jnp.sum(by_expert, axis=1)
    gate_grad = jnp.sum(jnp.where(onehot, by_expert[:, None, :], 0.0), axis=2)
    return (mixed, token_grad, gate_grad, grad_gate, grad_up, grad_down)


def body(tokens, routes, gates, cotangent, w_gate, w_up, w_down):
    token_count, top_k = routes.shape
    senders = lax.axis_size("expert")
    halves = lax.axis_size("half")
    capacity = 2 * token_count * top_k // (w_gate.shape[0] * senders)
    dense = capacity >= token_count and w_gate.shape[0] == 1
    if dense and halves == 2 and senders % 4 == 0 and token_count % 32 == 0:
        return dense_body(tokens, routes, gates, cotangent, w_gate, w_up, w_down)
    return slot_body(tokens, routes, gates, cotangent, w_gate, w_up, w_down)


def solution(mesh):
    placed = (
        P("expert", None),
        P("expert", None),
        P("expert", None),
        P("expert", None),
        P("expert", None, "half"),
        P("expert", None, "half"),
        P("expert", "half", None),
    )
    return jax.shard_map(
        body,
        mesh=mesh,
        in_specs=placed,
        out_specs=(
            P("expert", None),
            P("expert", None),
            P("expert", None),
            P("expert", None, "half"),
            P("expert", None, "half"),
            P("expert", "half", None),
        ),
        check_vma=False,
    )
```
